32 devices in a mesh: cols: 8 (over y, x, core), rows: 4 (over z).
Axes of the slice: x: 2, y: 2, z: 4, core: 2. Of those that a mesh axis runs over, the one named last changes fastest.
Arguments:
- weight: float32 [8192, 28672], P('rows', 'cols'), may hold values from -6 to 6
- scales: float32 [8192], P('rows'), may hold values from 0.2 to 0.5
- panels: float32 [1024, 28672], P('cols', 'rows')
- block_inverse: float32 [2, 128, 128], replicated
- grid_codes: int32 [16], replicated, may hold values from -12 to 12, as said below
- block_starts: int32 [2], replicated, may hold values from 0 to 25088, as said below
Outputs:
- result: float32 [8192, 28672], P('rows', 'cols')
The draws below stay inside these ranges and needn't reach their ends.
Inputs may be any that keep to these rules, and one draw needn't show every extreme that they name: `grid_codes`: strictly increasing. `block_starts`: strictly increasing multiples of 3584; the last block starts at the last device's columns.
All inputs are finite; a program needn't handle non-finite values.
Results may differ from the reference program's by a relative error of at most 0.00012.
Values sent between devices are 32-bit elements; how exact they have to be, the bound alone decides.
A program may use at most 192 MiB of HBM per device.

```python
import math
import jax
import jax.numpy as jnp
from jax import lax

OUT = 8192
COLS_IN = 28672
BLK = 128
SUB = 32
LEVELS = 16
BLOCKS = 2
COLS_DEV = 3584
PANELS = 1024
N_COLS = 8


def draw_panels(key, part):
    row_ids = jnp.arange(PANELS, dtype=jnp.int32)[:, None]
    column_ids = jnp.arange(COLS_IN, dtype=jnp.int32)[None, :]
    start_col = row_ids // BLK * COLS_DEV
    local_row = row_ids % BLK
    inside = column_ids - start_col
    noise = jax.random.normal(jax.random.fold_in(key, 11), (PANELS, COLS_IN), jnp.float32)
    diag_vals = jnp.exp(jax.random.uniform(jax.random.fold_in(key, 12), (PANELS, COLS_IN), jnp.float32, -0.7, 0.7))
    upper = jnp.where(inside > local_row, noise / BLK ** 0.5, 0.0)
    upper = jnp.where(inside == local_row, diag_vals, upper)
    values = jnp.where(inside >= BLK, 2.0 * noise / BLK ** 0.5, upper)
    values = jnp.where(inside < 0, 0.0, values)
    return values.astype(jnp.float32)


def draw_block_inverse(key, part):
    noise = jax.random.normal(jax.random.fold_in(key, 21), (BLOCKS, BLK, BLK), jnp.float32)
    diag_vals = jax.random.uniform(jax.random.fold_in(key, 22), (BLOCKS, BLK, BLK), jnp.float32, 0.5, 1.5)
    row_ids = jnp.arange(BLK, dtype=jnp.int32)[:, None]
    column_ids = jnp.arange(BLK, dtype=jnp.int32)[None, :]
    values = jnp.where(column_ids > row_ids, 0.6 * noise / BLK ** 0.5, 0.0)
    values = jnp.where(column_ids == row_ids, diag_vals, values)
    return values.astype(jnp.float32)


def draw_grid_codes(key, part):
    picked = jax.random.permutation(jax.random.fold_in(key, 31), 25)[:LEVELS]
    return (jnp.sort(picked) - 12).astype(jnp.int32)


def draw_block_starts(key, part):
    earlier = jnp.sort(jax.random.permutation(jax.random.fold_in(key, 41), N_COLS - 1)[:BLOCKS - 1])
    owners = jnp.concatenate([earlier.astype(jnp.int32), jnp.full((1,), N_COLS - 1, jnp.int32)])
    return (owners * COLS_DEV).astype(jnp.int32)


def block_scale(rng, dims, cuts, low, high):
    gain, own = 1.0, jax.random.fold_in(rng, 6)
    for axis_at, blocks in cuts:
        draws = jnp.exp(jax.random.uniform(jax.random.fold_in(own, axis_at), (blocks,), jnp.float32, low / len(cuts), high / len(cuts)))
        gain = gain * jnp.repeat(draws, dims[axis_at] // blocks).reshape([-1 if axis == axis_at else 1 for axis in range(len(dims))])
    return gain


def normal_values(rng, dims, width, reach, split=(), kind=jnp.bfloat16):
    values = width * jax.random.normal(rng, dims, jnp.float32)
    if split:
        values = values * block_scale(rng, dims, split, -0.22, 0.18)
    return jnp.clip(values, -reach, reach).astype(kind)


def setup_inputs(seed: int = 0) -> dict:
    arg_keys = jax.random.split(jax.random.key(seed), 7)
    return {
        "weight": normal_values(arg_keys[0], (OUT, COLS_IN), 1.0, 6.0, ((0, 4), (1, 8)), jnp.float32),
        "scales": jnp.clip(jnp.exp(math.log(0.5) - 0.9162907 * jax.random.uniform(arg_keys[1], (OUT,), jnp.float32) ** block_scale(arg_keys[1], (OUT,), ((0, 4),), -0.2, 0.2)), 0.2, 0.5),
        "panels": draw_panels(jax.random.fold_in(arg_keys[6], 71), 0),
        "block_inverse": draw_block_inverse(jax.random.fold_in(arg_keys[6], 71), 0),
        "grid_codes": draw_grid_codes(jax.random.fold_in(arg_keys[6], 71), 0),
        "block_starts": draw_block_starts(jax.random.fold_in(arg_keys[6], 71), 0),
    }


softness = 0.2


def quantize(values, scales, grid_codes):
    levels = grid_codes.astype(jnp.float32)
    ratio = values / scales[:, None]
    output = jnp.zeros_like(values) + levels[0]
    for level_id in range(LEVELS - 1):
        level_gap = levels[level_id + 1] - levels[level_id]
        midpoint = 0.5 * (levels[level_id] + levels[level_id + 1])
        output = output + level_gap * jax.nn.sigmoid((ratio - midpoint) / softness)
    return output * scales[:, None]


def inner_block(block_cols, diag_block, inverse, scales, grid_codes):
    local_ids = jnp.arange(BLK, dtype=jnp.int32)
    pieces = []
    for piece_id in range(BLK // SUB):
        low_col = piece_id * SUB
        current = block_cols[:, low_col:low_col + SUB]
        quantized = quantize(current, scales, grid_codes)
        error_part = jnp.dot(current - quantized, inverse[low_col:low_col + SUB, low_col:low_col + SUB], precision=lax.Precision.HIGHEST, preferred_element_type=jnp.float32)
        later_rows = jnp.where(local_ids[None, :] >= low_col + SUB, diag_block[low_col:low_col + SUB, :], 0.0)
        block_cols = block_cols - jnp.dot(error_part, later_rows, precision=lax.Precision.HIGHEST, preferred_element_type=jnp.float32)
        block_cols = block_cols.at[:, low_col:low_col + SUB].set(quantized)
        pieces.append(error_part)
    return block_cols, jnp.concatenate(pieces, axis=1)


def reference(weight, scales, panels, block_inverse, grid_codes, block_starts):
    cols_per = COLS_IN // N_COLS
    column_ids = jnp.arange(COLS_IN, dtype=jnp.int32)
    for block_id in range(BLOCKS):
        start_col = block_starts[block_id].astype(jnp.int32)
        owner_id = (start_col // cols_per).astype(jnp.int32)
        panel_rows = lax.dynamic_slice_in_dim(panels, (owner_id * BLK).astype(jnp.int32), BLK, 0)
        diag_block = lax.dynamic_slice_in_dim(panel_rows, start_col, BLK, 1)
        block_cols = lax.dynamic_slice_in_dim(weight, start_col, BLK, 1)
        block_cols, errors = inner_block(block_cols, diag_block, block_inverse[block_id], scales, grid_codes)
        weight = lax.dynamic_update_slice_in_dim(weight, block_cols, start_col, 1)
        trail_rows = jnp.where(column_ids[None, :] >= start_col + BLK, panel_rows, 0.0)
        weight = weight - jnp.dot(errors, trail_rows, precision=lax.Precision.HIGHEST, preferred_element_type=jnp.float32)
    return weight
```

```python
import functools

import jax
import jax.numpy as jnp
from jax import lax
from jax.experimental import pallas as pl
from jax.experimental.pallas import tpu as pltpu
from jax.sharding import PartitionSpec as P

BLK = 128
SUB = 32
LEVELS = 16
GROUPS = BLK // SUB
CH = 8
ETILE = 512

softness = 0.2
F32, BF16 = jnp.float32, jnp.bfloat16
MESH = pl.DeviceIdType.MESH


def split2(x):
    hi = x.astype(BF16)
    return hi, (x - hi.astype(F32)).astype(BF16)


def split3(x):
    hi = x.astype(BF16)
    rest = x - hi.astype(F32)
    mid = rest.astype(BF16)
    return hi, mid, (rest - mid.astype(F32)).astype(BF16)


def rounding_rows(inverse, diag_block):
    rows = lax.broadcasted_iota(jnp.int32, (BLK, BLK), 0) // SUB
    cols = lax.broadcasted_iota(jnp.int32, (BLK, BLK), 1) // SUB
    inv = jnp.where(rows == cols, inverse, 0.0)
    later = jnp.where(cols > rows, diag_block, 0.0)
    return inv + jnp.dot(
        inv, later, precision=lax.Precision.HIGHEST, preferred_element_type=F32
    )


def inner_block(block_t, scale, codes_ref, g_ref, b):
    levels = [codes_ref[k].astype(F32) for k in range(LEVELS)]
    sharp = 0.5 / softness
    center = 0.5 * (levels[0] + levels[LEVELS - 1])
    half = [0.5 * (levels[k + 1] - levels[k]) for k in range(LEVELS - 1)]
    mids = [sharp * 0.5 * (levels[k] + levels[k + 1]) for k in range(LEVELS - 1)]
    gain = sharp / scale
    groups = [block_t[j * SUB : (j + 1) * SUB, :] for j in range(GROUPS)]
    errors = []
    for j in range(GROUPS):
        current = groups[j]
        ratio = current * gain
        total = jnp.zeros_like(current) + center
        for k in range(LEVELS - 1):
            total = total + half[k] * jnp.tanh(ratio - mids[k])
        quantized = total * scale
        h, m, l = split3(current - quantized)
        stacked = jnp.concatenate([h, m, h, l, h, m, l, m], axis=0)
        moved = jnp.dot(g_ref[b, j], stacked, preferred_element_type=F32)
        errors.append(moved[j * SUB : (j + 1) * SUB, :])
        for i in range(j + 1, GROUPS):
            groups[i] = groups[i] - moved[i * SUB : (i + 1) * SUB, :]
        groups[j] = quantized
    return jnp.concatenate(groups, axis=0), jnp.concatenate(errors, axis=0)


def put_rounding(g_ref, b, inverse, diag):
    h, m, l = [piece.astype(F32) for piece in split3(rounding_rows(inverse, diag))]
    for j in range(GROUPS):
        at = slice(j * SUB, (j + 1) * SUB)
        stacked = jnp.concatenate(
            [h[at], h[at], m[at], h[at], l[at], m[at], m[at], l[at]], axis=0
        )
        g_ref[b, j] = stacked.T.astype(BF16)


def lookup(table, index):
    value = jnp.int32(table[0])
    for i in range(1, len(table)):
        value = jnp.where(index == i, jnp.int32(table[i]), value)
    return value


def move_kernel(
    o, N, R, codes_ref, inv_ref, scale_ref, pan_ref, w_ref,
    land, e0, e1, block, wv,
    gcat, diag, cross, xcat, wblk, rblk,
    rrecv, drecv, qrecv, up_s, dn_s, del_s, scat_s, qscat_s,
    era, erb, esa, esb, pa, pb, dsem, dsend, xsem, xsend, wrecv, wsend, bsem, lsem
):
    col, me = lax.axis_index("cols"), lax.axis_index("rows")
    cols_per = w_ref.shape[1]
    ratio = pan_ref.shape[1] // cols_per
    last = N - 1
    chips = N // 2
    m = BLK // chips // CH
    n_chunks = BLK // CH
    nt = w_ref.shape[0] // ETILE
    hpart = ETILE // 2
    oh, oq, lq = o // ratio, o // 2, chips - 1
    k0 = o % 2
    k1 = 1 - k0
    first_at, second_at = 2 * oq + k1, 2 * lq + k1
    q, k = col // 2, col % 2
    partner = q * 2 + 1 - k
    carrier = k == k0
    is_owner, is_last = col == o, col == last
    rounds_first, rounds_second = col == first_at, col == second_at

    barrier = pltpu.get_barrier_semaphore()
    for step in range(1, N):
        pl.semaphore_signal(
            barrier, inc=1, device_id=(lax.rem(col + step, N), me), device_id_type=MESH
        )
    for step in range(1, R):
        pl.semaphore_signal(
            barrier, inc=1, device_id=(col, lax.rem(me + step, R)), device_id_type=MESH
        )
    pl.semaphore_wait(barrier, N - 1 + R - 1)

    def both(*terms):
        value = terms[0]
        for term in terms[1:]:
            value = jnp.logical_and(value, term)
        return value

    def remote(src, dst, ssem, rsem, to):
        return pltpu.make_async_remote_copy(
            src_ref=src, dst_ref=dst, send_sem=ssem, recv_sem=rsem,
            device_id=to, device_id_type=MESH,
        )

    def rows_at(slot):
        return land.at[pl.ds(pl.multiple_of(slot * CH, CH), CH)]

    def slot0(chip, s, i):
        return jnp.where(chip * 2 + k0 == s, chip * m + i, 2 * n_chunks + s * m + i)

    def slot1(chip, i):
        own = chip * 2 + k0 == last
        return jnp.where(own, n_chunks + chip * m + i, 2 * n_chunks + N * m + i)

    def pan(j, kk):
        return pan_ref.at[pl.ds(pl.multiple_of(j * CH, CH), CH), pl.ds(kk * cols_per, cols_per)]

    def corner(kk):
        return pan_ref.at[:, pl.ds(kk * cols_per, BLK)]

    def first_cols():
        return w_ref.at[:, pl.ds(0, BLK)]

    to_first, to_second = (first_at, me), (second_at, me)
    w_first = remote(first_cols(), wblk.at[0], wsend.at[0], wrecv.at[0], to_first)
    d_first = remote(corner(o % ratio), diag.at[0], dsend.at[0], dsem.at[0], to_first)
    x_second = remote(corner(last % ratio), cross, xsend.at[0], xsem, to_second)
    if second_at == last:
        w_second = pltpu.make_async_copy(first_cols(), wblk.at[1], wrecv.at[1])
        d_second = pltpu.make_async_copy(corner(last % ratio), diag.at[1], dsem.at[1])
    else:
        w_second = remote(first_cols(), wblk.at[1], wsend.at[1], wrecv.at[1], to_second)
        d_second = remote(corner(last % ratio), diag.at[1], dsend.at[R], dsem.at[1], to_second)

    def pass_on(ref, ssem, rsem, step):
        return remote(ref, ref, ssem, rsem, (col, lax.rem(me + step, R)))

    def pass_diag(b, step):
        return pass_on(diag.at[b], dsend.at[b * R + step], dsem.at[b], step)

    def pass_cross(step):
        return pass_on(cross, xsend.at[step], xsem, step)

    def arrived(ref, sem):
        return remote(ref, ref, dsend.at[0], sem, (partner, me))

    top = me == R - 1

    @pl.when(both(is_owner, me == oh))
    def _():
        d_first.start()

    @pl.when(is_owner)
    def _():
        w_first.start()

    @pl.when(both(is_owner, top))
    def _():
        x_second.start()

    @pl.when(both(is_last, top))
    def _():
        d_second.start()

    @pl.when(is_last)
    def _():
        w_second.start()

    flows = ratio * m

    def scatter(chip, n):
        kk, i = lax.rem(n, ratio), n // ratio
        s = me * ratio + kk
        return (chip * m + i, kk, rows_at(slot0(chip, s, i)), s * m + i)

    def scatter_to(chip, n):
        j, kk, dst, f = scatter(chip, n)
        return remote(
            pan_at(j, kk), dst, scat_s.at[n * chips + chip], rrecv.at[f], (chip * 2 + k0, me)
        )

    def scatter_own(n):
        j, kk, dst, f = scatter(oq, n)
        return pltpu.make_async_copy(pan_at(j, kk), dst, rrecv.at[f])

    def pan_at(j, kk):
        return pan_ref.at[
            pl.ds(pl.multiple_of(j * CH, CH), CH),
            pl.ds(pl.multiple_of(kk * cols_per, BLK), cols_per),
        ]

    def scatter1(chip, i):
        return remote(
            pan(chip * m + i, last % ratio), rows_at(slot1(chip, i)),
            qscat_s.at[i * chips + chip], rrecv.at[N * m + i], (chip * 2 + k0, me),
        )

    def scatter1_own(i):
        return pltpu.make_async_copy(
            pan(lq * m + i, last % ratio), rows_at(slot1(lq, i)), rrecv.at[N * m + i]
        )

    p1_local = pltpu.make_async_copy(
        pan_ref.at[:, pl.ds((last % ratio) * cols_per, cols_per)],
        land.at[pl.ds(BLK, BLK)], lsem.at[1],
    )

    def own_row(j):
        return pltpu.make_async_copy(pan(j, o % ratio), rows_at(j), drecv.at[j])

    @pl.when(is_owner)
    def _():
        @pl.loop(0, flows)
        def _(n):
            @pl.when(me * ratio + lax.rem(n, ratio) >= o)
            def _():
                scatter_own(n).start()

                @pl.loop(1, chips)
                def _(step):
                    scatter_to(lax.rem(oq + step, chips), n).start()

        @pl.when(me == oh)
        def _():
            for j in range(n_chunks):
                if j // m != oq:
                    own_row(j).start()

    @pl.when(both(is_last, top))
    def _():
        p1_local.start()

        @pl.loop(0, m)
        def _(i):
            if k0 == 0:
                scatter1(lq, i).start()

            @pl.loop(1, chips)
            def _(step):
                scatter1(lax.rem(lq + step, chips), i).start()

    wcopy = pltpu.make_async_copy(w_ref, wv, lsem.at[0])
    wcopy.start()

    order = [c ^ (c >> 1) for c in range(chips)]
    where = [order.index(c) for c in range(chips)]
    pos = lookup(where, q)
    spot = lax.rem(pos - where[oq] + chips, chips)
    fwd_chip = lookup(order, lax.rem(pos + 1, chips))
    bwd_chip = lookup(order, lax.rem(pos + chips - 1, chips))
    ends = (chips - 1, 1)

    def epart(t, half):
        return e0.at[pl.ds(pl.multiple_of(t * ETILE + half * hpart, hpart), hpart)]

    def ring(t, half):
        to = fwd_chip if half == 0 else bwd_chip
        ss, rs = (esa, era) if half == 0 else (esb, erb)
        return remote(epart(t, half), epart(t, half), ss.at[t], rs.at[t], (to * 2 + k, me))

    def across(t, half):
        ss, rs = (pa, era) if half == 0 else (pb, erb)
        return remote(epart(t, half), epart(t, half), ss.at[t], rs.at[t], (partner, me))

    def send_errors(t):
        for half in range(2):
            ring(t, half).start()
            across(t, half).start()

    b_first = remote(rblk.at[0], block, bsem.at[0], bsem.at[1], (o, me))
    e_second = remote(e1, e1, bsem.at[2], bsem.at[3], (last, me))
    b_second = remote(rblk.at[1], block, bsem.at[4], bsem.at[5], (last, me))

    @pl.when(rounds_first)
    def _():
        arrived(diag.at[0], dsem.at[0]).wait_recv()

        @pl.when(me == oh)
        def _():
            for step in range(1, R):
                pass_diag(0, step).start()

        w_first.wait_recv()

    @pl.when(rounds_second)
    def _():
        arrived(diag.at[1], dsem.at[1]).wait_recv()
        arrived(cross, xsem).wait_recv()

        @pl.when(top)
        def _():
            for step in range(1, R):
                pass_diag(1, step).start()
                pass_cross(step).start()

        arrived(wblk.at[1], wrecv.at[1]).wait_recv()
        xh, xl = split2(cross[...])
        xcat[...] = jnp.concatenate([xh, xh, xl], axis=0)

    @pl.loop(0, 2)
    def _(b):
        @pl.when(jnp.logical_or(both(b == 0, rounds_first), both(b == 1, rounds_second)))
        def _():
            put_rounding(gcat, b, inv_ref[b], diag[b])

    lag = jnp.where(rounds_first, 0, jnp.maximum(spot, chips - spot))

    def relay_errors(t, half):
        @pl.when(both(t >= 0, t < nt))
        def _():
            ring(t, half).wait_recv()

            @pl.when(spot != ends[half])
            def _():
                ring(t, half).start()

            across(t, half).start()

    @pl.when(jnp.logical_not(carrier))
    def _():
        @pl.loop(0, 2 * (nt + chips))
        def _(turn):
            now, b = turn // 2, lax.rem(turn, 2)
            t = jnp.where(b == 0, now, now - lag)
            inside = both(t >= 0, t < nt)
            at = pl.ds(pl.multiple_of(t * ETILE, ETILE), ETILE)

            @pl.when(both(b == 1, jnp.logical_not(rounds_first)))
            def _():
                relay_errors(now - spot, 0)
                relay_errors(now - chips + spot, 1)

            @pl.when(both(b == 1, rounds_second, inside))
            def _():
                eh, el = split2(e0[at, :])
                wblk[1, at, :] = wblk[1, at, :] - jnp.dot(
                    jnp.concatenate([eh, el, eh], axis=1), xcat[...], preferred_element_type=F32
                )

            mine = jnp.logical_or(both(b == 0, rounds_first), both(b == 1, rounds_second))

            @pl.when(both(mine, inside))
            def _():
                rounded, errors = inner_block(
                    wblk[b, at, :].T, scale_ref[:, at], codes_ref, gcat, b
                )
                rblk[b, at, :] = rounded.T
                errors = errors.T

                @pl.when(b == 0)
                def _():
                    e0[at, :] = errors

                @pl.when(b == 1)
                def _():
                    e1[at, :] = errors

            @pl.when(both(b == 1, rounds_first, now > 0, now <= nt))
            def _():
                send_errors(now - 1)

    @pl.when(rounds_first)
    def _():
        b_first.start()

    @pl.when(rounds_second)
    def _():
        if second_at != last:
            e_second.start()
            b_second.start()
        else:
            block[...] = rblk[1]

    def relay(n, d, sign):
        kk, i = lax.rem(n, ratio), n // ratio
        h = me + sign * d
        s = h * ratio + kk
        f = s * m + i
        valid = both(n >= 0, n < flows, s >= o)
        if sign < 0:
            valid = both(valid, h >= 0)
        if sign > 0:
            valid = both(valid, h < R)
        buf = rows_at(slot0(q, s, i))

        def hop(sem, step):
            return remote(buf, buf, sem.at[f], rrecv.at[f], (col, me + step))

        deliver = remote(
            buf, rows_at(q * m + i), del_s.at[f], drecv.at[q * m + i], (s, me)
        )
        goes = col != s
        if sign == 0:
            goes = both(goes, jnp.logical_or(s != o, me != oh))
        return valid, goes, hop(up_s, 1), hop(dn_s, -1), deliver

    def relay_start(n, d, sign):
        valid, goes, up, down, deliver = relay(n, d, sign)

        @pl.when(valid)
        def _():
            up.wait_recv()
            if sign <= 0:
                @pl.when(me < R - 1)
                def _():
                    up.start()
            if sign >= 0:
                @pl.when(me > 0)
                def _():
                    down.start()

            @pl.when(goes)
            def _():
                deliver.start()

    def relay_end(n, d, sign):
        valid, goes, up, down, deliver = relay(n, d, sign)

        @pl.when(valid)
        def _():
            if sign <= 0:
                @pl.when(me < R - 1)
                def _():
                    up.wait_send()
            if sign >= 0:
                @pl.when(me > 0)
                def _():
                    down.wait_send()

            @pl.when(goes)
            def _():
                deliver.wait_send()

    def relay1(i):
        f = N * m + i
        buf = rows_at(slot1(q, i))
        down = remote(buf, buf, dn_s.at[f], rrecv.at[f], (col, me - 1))
        deliver = remote(
            buf, rows_at(n_chunks + q * m + i), del_s.at[f], qrecv.at[q * m + i], (last, me)
        )
        return down, deliver, both(me < R - 1, col != last)

    at_source = both(is_last, top)

    def relay1_start(i):
        down, deliver, goes = relay1(i)

        @pl.when(jnp.logical_not(at_source))
        def _():
            down.wait_recv()

        @pl.when(both(at_source, i == 0))
        def _():
            p1_local.wait()

        @pl.when(me > 0)
        def _():
            down.start()

        @pl.when(goes)
        def _():
            deliver.start()

    def relay1_end(i):
        down, deliver, goes = relay1(i)

        @pl.when(me > 0)
        def _():
            down.wait_send()

        @pl.when(goes)
        def _():
            deliver.wait_send()

    def walk(one, other):
        @pl.loop(0, flows + 2 * R)
        def _(level):
            for d in range(R):
                for sign in (0,) if d == 0 else (-1, 1):
                    one(level - d, d, sign)
            turn = level - (R - 1 - me)

            @pl.when(both(turn >= 0, lax.rem(turn + 2 * R, 2) == 0, turn < 2 * m))
            def _():
                other(turn // 2)

    @pl.when(carrier)
    def _():
        walk(relay_start, relay1_start)
        walk(relay_end, relay1_end)

    @pl.when(jnp.logical_not(carrier))
    def _():
        @pl.loop(0, nt)
        def _(t):
            for half in range(2):
                @pl.when(jnp.logical_or(rounds_first, spot != ends[half]))
                def _():
                    ring(t, half).wait_send()

                across(t, half).wait_send()

    @pl.when(carrier)
    def _():
        @pl.loop(0, nt)
        def _(t):
            for half in range(2):
                across(t, half).wait_recv()

    @pl.when(is_owner)
    def _():
        w_first.wait_send()
        b_first.wait_recv()

        @pl.loop(0, flows)
        def _(n):
            @pl.when(me * ratio + lax.rem(n, ratio) >= o)
            def _():
                @pl.loop(1, chips)
                def _(step):
                    scatter_to(lax.rem(oq + step, chips), n).wait_send()

    @pl.when(both(is_owner, me == oh))
    def _():
        d_first.wait_send()

    @pl.when(both(is_owner, top))
    def _():
        x_second.wait_send()

    @pl.when(rounds_first)
    def _():
        b_first.wait_send()

        @pl.when(me == oh)
        def _():
            for step in range(1, R):
                pass_diag(0, step).wait_send()

    @pl.when(both(rounds_second, top))
    def _():
        for step in range(1, R):
            pass_diag(1, step).wait_send()
            pass_cross(step).wait_send()

    if second_at != last:
        @pl.when(rounds_second)
        def _():
            e_second.wait_send()
            b_second.wait_send()

        @pl.when(is_last)
        def _():
            w_second.wait_send()
            e_second.wait_recv()
            b_second.wait_recv()

        @pl.when(both(is_last, top))
        def _():
            d_second.wait_send()

    @pl.when(both(is_last, top))
    def _():
        if k0 == 0:
            p1_local.wait()

        @pl.loop(0, m)
        def _(i):
            if k0 == 0:
                scatter1(lq, i).wait_send()

            @pl.loop(1, chips)
            def _(step):
                scatter1(lax.rem(lq + step, chips), i).wait_send()

    @pl.loop(0, n_chunks)
    def _(j):
        carried = (j // m) * 2 + k0

        @pl.when(both(col >= o, col != carried))
        def _():
            arrived(rows_at(j), drecv.at[j]).wait_recv()

        @pl.when(both(is_last, me < R - 1, carried != last))
        def _():
            arrived(rows_at(n_chunks + j), qrecv.at[j]).wait_recv()

    wcopy.wait()


def move(o, N, R, codes, inverse, scales, panels, weight):
    rows, cols_per = weight.shape
    chips = N // 2
    m = BLK // chips // CH
    ratio = panels.shape[1] // cols_per
    n_chunks = BLK // CH
    n_rel = (N + 1) * m
    nt = rows // ETILE
    hbm = pl.BlockSpec(memory_space=pltpu.HBM)
    vmem = pl.BlockSpec(memory_space=pltpu.VMEM)
    smem = pl.BlockSpec(memory_space=pltpu.SMEM)
    dma = pltpu.SemaphoreType.DMA
    return pl.pallas_call(
        functools.partial(move_kernel, o, N, R),
        out_shape=(
            pltpu.VMEM((2 * BLK + n_rel * CH, cols_per), F32),
            pltpu.VMEM((rows, BLK), F32),
            pltpu.VMEM((rows, BLK), F32),
            pltpu.VMEM((rows, BLK), F32),
            pltpu.VMEM((rows, cols_per), F32),
        ),
        in_specs=[smem, vmem, vmem, hbm, hbm],
        out_specs=(vmem,) * 5,
        scratch_shapes=[
            pltpu.VMEM((2, GROUPS, BLK, 8 * SUB), BF16),
            pltpu.VMEM((2, BLK, BLK), F32),
            pltpu.VMEM((BLK, BLK), F32),
            pltpu.VMEM((3 * BLK, BLK), BF16),
            pltpu.VMEM((2, rows, BLK), F32),
            pltpu.VMEM((2, rows, BLK), F32),
            dma((n_rel,)), dma((n_chunks,)), dma((n_chunks,)),
            dma((n_rel,)), dma((n_rel,)), dma((n_rel,)),
            dma((ratio * m * chips,)), dma((m * chips,)),
            dma((nt,)), dma((nt,)), dma((nt,)), dma((nt,)), dma((nt,)), dma((nt,)),
            dma((2,)), dma((2 * R,)), dma, dma((R,)), dma((2,)), dma((2,)), dma((6,)), dma((2,)),
        ],
        compiler_params=pltpu.CompilerParams(
            collective_id=o + 1, has_side_effects=True, vmem_limit_bytes=20 * 1024 * 1024
        ),
        name=f"move_{o}",
    )(codes, inverse, scales[None, :], panels, weight)


def apply_kernel(o, N, col_ref, land, e0, e1, block, wv, out_ref, pcat, ecat, obuf, sems):
    rows, cols_per = wv.shape
    tile = obuf.shape[1]
    chunk = obuf.shape[2]
    slots = obuf.shape[0]
    col = col_ref[0]
    is_owner = col == o
    is_last = col == N - 1
    touched = col >= o
    nr, nc = rows // tile, cols_per // chunk

    def put_panel(b):
        @pl.loop(0, nc)
        def _(i):
            at = pl.ds(pl.multiple_of(i * chunk, chunk), chunk)
            hi, lo = split2(land[b * BLK : (b + 1) * BLK, at])
            pcat[3 * b * BLK : (3 * b + 1) * BLK, at] = hi
            pcat[(3 * b + 1) * BLK : (3 * b + 2) * BLK, at] = hi
            pcat[(3 * b + 2) * BLK : (3 * b + 3) * BLK, at] = lo

    def clear_panel(b):
        pcat[3 * b * BLK : (3 * b + 3) * BLK, :BLK] = jnp.zeros((3 * BLK, BLK), BF16)

    def put_errors(b, ref):
        hi, lo = split2(ref[...])
        ecat[:, 3 * b * BLK : (3 * b + 1) * BLK] = hi
        ecat[:, (3 * b + 1) * BLK : (3 * b + 2) * BLK] = lo
        ecat[:, (3 * b + 2) * BLK : (3 * b + 3) * BLK] = hi

    @pl.when(touched)
    def _():
        put_panel(0)
        put_errors(0, e0)

    @pl.when(is_owner)
    def _():
        clear_panel(0)

    @pl.when(is_last)
    def _():
        put_panel(1)
        clear_panel(1)
        put_errors(1, e1)

    def out_copy(step):
        slot = lax.rem(step, slots)
        c, r = step // nr, lax.rem(step, nr)
        return pltpu.make_async_copy(
            obuf.at[slot],
            out_ref.at[
                pl.ds(pl.multiple_of(r * tile, tile), tile),
                pl.ds(pl.multiple_of(c * chunk, chunk), chunk),
            ],
            sems.at[slot],
        )

    @pl.loop(0, nr * nc)
    def _(step):
        slot = lax.rem(step, slots)
        c, r = step // nr, lax.rem(step, nr)
        at_r = pl.ds(pl.multiple_of(r * tile, tile), tile)
        at_c = pl.ds(pl.multiple_of(c * chunk, chunk), chunk)

        @pl.when(step >= slots)
        def _():
            out_copy(step - slots).wait()

        @pl.when(is_last)
        def _():
            obuf[slot] = wv[at_r, at_c] - jnp.dot(
                ecat[at_r, :], pcat[:, at_c], preferred_element_type=F32
            )

        @pl.when(jnp.logical_and(touched, jnp.logical_not(is_last)))
        def _():
            obuf[slot] = wv[at_r, at_c] - jnp.dot(
                ecat[at_r, : 3 * BLK], pcat[: 3 * BLK, at_c], preferred_element_type=F32
            )

        @pl.when(jnp.logical_not(touched))
        def _():
            obuf[slot] = wv[at_r, at_c]

        @pl.when(jnp.logical_and(c == 0, jnp.logical_or(is_owner, is_last)))
        def _():
            obuf[slot, :, :BLK] = block[at_r, :]

        out_copy(step).start()

    for k in range(slots):
        out_copy(nr * nc - slots + k).wait()


def apply(o, N, col, land, e0, e1, block, wv):
    rows, cols_per = wv.shape
    tile = next(t for t in (512, 256, 128, 64, 32, 16, 8) if rows % t == 0)
    chunk = next(c for c in (512, 256, 128) if cols_per % c == 0)
    slots = 4
    vmem = pl.BlockSpec(memory_space=pltpu.VMEM)
    return pl.pallas_call(
        functools.partial(apply_kernel, o, N),
        out_shape=pltpu.HBM((rows, cols_per), F32),
        in_specs=[pl.BlockSpec(memory_space=pltpu.SMEM)] + [vmem] * 5,
        out_specs=pl.BlockSpec(memory_space=pltpu.HBM),
        scratch_shapes=[
            pltpu.VMEM((6 * BLK, cols_per), BF16),
            pltpu.VMEM((rows, 6 * BLK), BF16),
            pltpu.VMEM((slots, tile, chunk), F32),
            pltpu.SemaphoreType.DMA((slots,)),
        ],
        compiler_params=pltpu.CompilerParams(vmem_limit_bytes=22 * 1024 * 1024),
        name=f"apply_{o}",
    )(col, land, e0, e1, block, wv)


def local(N, R, weight, scales, panels, block_inverse, grid_codes, block_starts):
    cols_per = weight.shape[1]
    owner = block_starts[0] // cols_per

    def branch(o):
        def run(weight, scales, panels, inverse, codes):
            parts = move(o, N, R, codes, inverse, scales, panels, weight)
            col = lax.axis_index("cols").astype(jnp.int32)[None]
            parts = [pltpu.with_memory_space_constraint(x, pltpu.VMEM) for x in parts]
            return apply(o, N, col, *parts)
        return run

    return lax.switch(
        owner, [branch(o) for o in range(N - 1)],
        weight, scales, panels, block_inverse, grid_codes,
    )


def solution(mesh):
    N, R = mesh.shape["cols"], mesh.shape["rows"]
    placed = (P("rows", "cols"), P("rows"), P("cols", "rows"), P(), P(), P())
    return jax.shard_map(
        functools.partial(local, N, R), mesh=mesh, in_specs=placed,
        out_specs=P("rows", "cols"), check_vma=False,
    )
```

```python
import functools

import jax
import jax.numpy as jnp
from jax import lax
from jax.experimental import pallas as pl
from jax.experimental.pallas import tpu as pltpu
from jax.sharding import PartitionSpec as P

BLK = 128
SUB = 32
LEVELS = 16
GROUPS = BLK // SUB
CH = 8
ETILE = 512

softness = 0.2
F32, BF16 = jnp.float32, jnp.bfloat16
MESH = pl.DeviceIdType.MESH


def split2(x):
    hi = x.astype(BF16)
    return hi, (x - hi.astype(F32)).astype(BF16)


def split3(x):
    hi = x.astype(BF16)
    rest = x - hi.astype(F32)
    mid = rest.astype(BF16)
    return hi, mid, (rest - mid.astype(F32)).astype(BF16)


def rounding_rows(inverse, diag_block):
    rows = lax.broadcasted_iota(jnp.int32, (BLK, BLK), 0) // SUB
    cols = lax.broadcasted_iota(jnp.int32, (BLK, BLK), 1) // SUB
    inv = jnp.where(rows == cols, inverse, 0.0)
    later = jnp.where(cols > rows, diag_block, 0.0)
    return inv + jnp.dot(
        inv, later, precision=lax.Precision.HIGHEST, preferred_element_type=F32
    )


def inner_block(block_t, scale, codes_ref, g_ref, b):
    levels = [codes_ref[k].astype(F32) for k in range(LEVELS)]
    sharp = 0.5 / softness
    center = 0.5 * (levels[0] + levels[LEVELS - 1])
    half = [0.5 * (levels[k + 1] - levels[k]) for k in range(LEVELS - 1)]
    mids = [sharp * 0.5 * (levels[k] + levels[k + 1]) for k in range(LEVELS - 1)]
    gain = sharp / scale
    groups = [block_t[j * SUB : (j + 1) * SUB, :] for j in range(GROUPS)]
    errors = []
    for j in range(GROUPS):
        current = groups[j]
        ratio = current * gain
        total = jnp.zeros_like(current) + center
        for k in range(LEVELS - 1):
            total = total + half[k] * jnp.tanh(ratio - mids[k])
        quantized = total * scale
        h, m, l = split3(current - quantized)
        stacked = jnp.concatenate([h, m, h, l, h, m, l, m], axis=0)
        moved = jnp.dot(g_ref[b, j], stacked, preferred_element_type=F32)
        errors.append(moved[j * SUB : (j + 1) * SUB, :])
        for i in range(j + 1, GROUPS):
            groups[i] = groups[i] - moved[i * SUB : (i + 1) * SUB, :]
        groups[j] = quantized
    return jnp.concatenate(groups, axis=0), jnp.concatenate(errors, axis=0)


def put_rounding(g_ref, b, inverse, diag):
    h, m, l = [piece.astype(F32) for piece in split3(rounding_rows(inverse, diag))]
    for j in range(GROUPS):
        at = slice(j * SUB, (j + 1) * SUB)
        stacked = jnp.concatenate(
            [h[at], h[at], m[at], h[at], l[at], m[at], m[at], l[at]], axis=0
        )
        g_ref[b, j] = stacked.T.astype(BF16)


def lookup(table, index):
    value = jnp.int32(table[0])
    for i in range(1, len(table)):
        value = jnp.where(index == i, jnp.int32(table[i]), value)
    return value


def move_kernel(
    o, N, R, codes_ref, inv_ref, scale_ref, pan_ref, w_ref,
    land, e0, e1, block, wv,
    gcat, diag, cross, xcat, wblk, rblk,
    rrecv, drecv, qrecv, up_s, dn_s, del_s, scat_s, qscat_s,
    era, erb, esa, esb, pa, pb, es2, er2, bs2, br2, dsem, dsend, xsem, xsend, wrecv, wsend, bsem, lsem
):
    col, me = lax.axis_index("cols"), lax.axis_index("rows")
    cols_per = w_ref.shape[1]
    ratio = pan_ref.shape[1] // cols_per
    last = N - 1
    chips = N // 2
    m = BLK // chips // CH
    n_chunks = BLK // CH
    nt = w_ref.shape[0] // ETILE
    hpart = ETILE // 2
    oh, oq, lq = o // ratio, o // 2, chips - 1
    m1 = n_chunks // 2
    nq = lq ^ (chips // 2 if oq == lq else 1)
    k0 = o % 2
    k1 = 1 - k0
    first_at, second_at = 2 * oq + k1, 2 * lq + k1
    q, k = col // 2, col % 2
    partner = q * 2 + 1 - k
    carrier = k == k0
    is_owner, is_last = col == o, col == last
    rounds_first, rounds_second = col == first_at, col == second_at

    barrier = pltpu.get_barrier_semaphore()
    for step in range(1, N):
        pl.semaphore_signal(
            barrier, inc=1, device_id=(lax.rem(col + step, N), me), device_id_type=MESH
        )
    for step in range(1, R):
        pl.semaphore_signal(
            barrier, inc=1, device_id=(col, lax.rem(me + step, R)), device_id_type=MESH
        )
    pl.semaphore_wait(barrier, N - 1 + R - 1)

    def both(*terms):
        value = terms[0]
        for term in terms[1:]:
            value = jnp.logical_and(value, term)
        return value

    def remote(src, dst, ssem, rsem, to):
        return pltpu.make_async_remote_copy(
            src_ref=src, dst_ref=dst, send_sem=ssem, recv_sem=rsem,
            device_id=to, device_id_type=MESH,
        )

    def rows_at(slot):
        return land.at[pl.ds(pl.multiple_of(slot * CH, CH), CH)]

    def slot0(chip, s, i):
        return jnp.where(chip * 2 + k0 == s, chip * m + i, 2 * n_chunks + s * m + i)

    def slot1(side, i):
        if k0 == 1:
            return jnp.where(side == 0, n_chunks + i, 2 * n_chunks + N * m + i)
        return 2 * n_chunks + N * m + i

    def pan(j, kk):
        return pan_ref.at[pl.ds(pl.multiple_of(j * CH, CH), CH), pl.ds(kk * cols_per, cols_per)]

    def corner(kk):
        return pan_ref.at[:, pl.ds(kk * cols_per, BLK)]

    def first_cols():
        return w_ref.at[:, pl.ds(0, BLK)]

    to_first, to_second = (first_at, me), (second_at, me)
    w_first = remote(first_cols(), wblk.at[0], wsend.at[0], wrecv.at[0], to_first)
    d_first = remote(corner(o % ratio), diag.at[0], dsend.at[0], dsem.at[0], to_first)
    x_second = remote(corner(last % ratio), cross, xsend.at[0], xsem, to_second)
    if second_at == last:
        w_second = pltpu.make_async_copy(first_cols(), wblk.at[1], wrecv.at[1])
        d_second = pltpu.make_async_copy(corner(last % ratio), diag.at[1], dsem.at[1])
    else:
        w_second = remote(first_cols(), wblk.at[1], wsend.at[1], wrecv.at[1], to_second)
        d_second = remote(corner(last % ratio), diag.at[1], dsend.at[R], dsem.at[1], to_second)

    def pass_on(ref, ssem, rsem, step):
        return remote(ref, ref, ssem, rsem, (col, lax.rem(me + step, R)))

    def pass_diag(b, step):
        return pass_on(diag.at[b], dsend.at[b * R + step], dsem.at[b], step)

    def pass_cross(step):
        return pass_on(cross, xsend.at[step], xsem, step)

    def arrived(ref, sem):
        return remote(ref, ref, dsend.at[0], sem, (partner, me))

    top = me == R - 1

    @pl.when(both(is_owner, me == oh))
    def _():
        d_first.start()

    @pl.when(is_owner)
    def _():
        w_first.start()

    @pl.when(both(is_owner, top))
    def _():
        x_second.start()

    @pl.when(both(is_last, top))
    def _():
        d_second.start()

    @pl.when(is_last)
    def _():
        w_second.start()

    flows = ratio * m

    def scatter(chip, n):
        kk, i = lax.rem(n, ratio), n // ratio
        s = me * ratio + kk
        return (chip * m + i, kk, rows_at(slot0(chip, s, i)), s * m + i)

    def scatter_to(chip, n):
        j, kk, dst, f = scatter(chip, n)
        return remote(
            pan_at(j, kk), dst, scat_s.at[n * chips + chip], rrecv.at[f], (chip * 2 + k0, me)
        )

    def scatter_own(n):
        j, kk, dst, f = scatter(oq, n)
        return pltpu.make_async_copy(pan_at(j, kk), dst, rrecv.at[f])

    def pan_at(j, kk):
        return pan_ref.at[
            pl.ds(pl.multiple_of(j * CH, CH), CH),
            pl.ds(pl.multiple_of(kk * cols_per, BLK), cols_per),
        ]

    def scatter1(side, i):
        return remote(
            pan(side * m1 + i, last % ratio), rows_at(slot1(side, i)),
            qscat_s.at[i * 2 + side], rrecv.at[N * m + i], ((lq, nq)[side] * 2 + k0, me),
        )

    p1_local = pltpu.make_async_copy(
        pan_ref.at[:, pl.ds((last % ratio) * cols_per, cols_per)],
        land.at[pl.ds(BLK, BLK)], lsem.at[1],
    )

    def own_row(j):
        return pltpu.make_async_copy(pan(j, o % ratio), rows_at(j), drecv.at[j])

    @pl.when(is_owner)
    def _():
        @pl.loop(0, flows)
        def _(n):
            @pl.when(me * ratio + lax.rem(n, ratio) >= o)
            def _():
                scatter_own(n).start()

                @pl.loop(1, chips)
                def _(step):
                    scatter_to(lax.rem(oq + step, chips), n).start()

        @pl.when(me == oh)
        def _():
            for j in range(n_chunks):
                if j // m != oq:
                    own_row(j).start()

    @pl.when(both(is_last, top))
    def _():
        p1_local.start()

        @pl.loop(0, m1)
        def _(i):
            if k0 == 0:
                scatter1(0, i).start()
            scatter1(1, i).start()

    wcopy = pltpu.make_async_copy(w_ref, wv, lsem.at[0])
    wcopy.start()

    order = [c ^ (c >> 1) for c in range(chips)]
    where = [order.index(c) for c in range(chips)]
    pos = lookup(where, q)
    spot = lax.rem(pos - where[oq] + chips, chips)
    fwd_chip = lookup(order, lax.rem(pos + 1, chips))
    bwd_chip = lookup(order, lax.rem(pos + chips - 1, chips))
    ends = (chips - 1, 1)

    def epart(t, half):
        return e0.at[pl.ds(pl.multiple_of(t * ETILE + half * hpart, hpart), hpart)]

    def ring(t, half):
        to = fwd_chip if half == 0 else bwd_chip
        ss, rs = (esa, era) if half == 0 else (esb, erb)
        return remote(epart(t, half), epart(t, half), ss.at[t], rs.at[t], (to * 2 + k, me))

    def across(t, half):
        ss, rs = (pa, era) if half == 0 else (pb, erb)
        return remote(epart(t, half), epart(t, half), ss.at[t], rs.at[t], (partner, me))

    def send_errors(t):
        for half in range(2):
            ring(t, half).start()
            across(t, half).start()

    b_first = remote(rblk.at[0], block, bsem.at[0], bsem.at[1], (o, me))
    def tile_of(ref, t):
        return ref.at[pl.ds(pl.multiple_of(t * ETILE, ETILE), ETILE)]

    def e_second(t):
        return remote(tile_of(e1, t), tile_of(e1, t), es2.at[t], er2.at[t], (last, me))

    def b_second(t):
        return remote(
            tile_of(rblk.at[1], t), tile_of(block, t), bs2.at[t], br2.at[t], (last, me)
        )

    @pl.when(rounds_first)
    def _():
        arrived(diag.at[0], dsem.at[0]).wait_recv()

        @pl.when(me == oh)
        def _():
            for step in range(1, R):
                pass_diag(0, step).start()

        w_first.wait_recv()

    @pl.when(rounds_second)
    def _():
        arrived(diag.at[1], dsem.at[1]).wait_recv()
        arrived(cross, xsem).wait_recv()

        @pl.when(top)
        def _():
            for step in range(1, R):
                pass_diag(1, step).start()
                pass_cross(step).start()

        arrived(wblk.at[1], wrecv.at[1]).wait_recv()
        xh, xl = split2(cross[...])
        xcat[...] = jnp.concatenate([xh, xh, xl], axis=0)

    @pl.loop(0, 2)
    def _(b):
        @pl.when(jnp.logical_or(both(b == 0, rounds_first), both(b == 1, rounds_second)))
        def _():
            put_rounding(gcat, b, inv_ref[b], diag[b])

    lag = jnp.where(rounds_first, 0, jnp.maximum(spot, chips - spot))

    def relay_errors(t, half):
        @pl.when(both(t >= 0, t < nt))
        def _():
            ring(t, half).wait_recv()

            @pl.when(spot != ends[half])
            def _():
                ring(t, half).start()

            across(t, half).start()

    @pl.when(jnp.logical_not(carrier))
    def _():
        @pl.loop(0, 2 * (nt + chips) + 1)
        def _(turn):
            now, b = turn // 2, lax.rem(turn, 2)
            t = jnp.where(b == 0, now, now - lag)
            inside = both(t >= 0, t < nt)
            at = pl.ds(pl.multiple_of(t * ETILE, ETILE), ETILE)

            @pl.when(both(b == 1, jnp.logical_not(rounds_first)))
            def _():
                relay_errors(now - spot, 0)
                relay_errors(now - chips + spot, 1)

            @pl.when(both(b == 1, rounds_second, inside))
            def _():
                eh, el = split2(e0[at, :])
                wblk[1, at, :] = wblk[1, at, :] - jnp.dot(
                    jnp.concatenate([eh, el, eh], axis=1), xcat[...], preferred_element_type=F32
                )

            mine = jnp.logical_or(both(b == 0, rounds_first), both(b == 1, rounds_second))

            @pl.when(both(mine, inside))
            def _():
                rounded, errors = inner_block(
                    wblk[b, at, :].T, scale_ref[:, at], codes_ref, gcat, b
                )
                rblk[b, at, :] = rounded.T
                errors = errors.T

                @pl.when(b == 0)
                def _():
                    e0[at, :] = errors

                @pl.when(b == 1)
                def _():
                    e1[at, :] = errors

            if second_at != last:
                @pl.when(both(b == 0, rounds_second, now > lag, now <= lag + nt))
                def _():
                    e_second(now - lag - 1).start()
                    b_second(now - lag - 1).start()

            @pl.when(both(b == 1, rounds_first, now > 0, now <= nt))
            def _():
                send_errors(now - 1)

    @pl.when(rounds_first)
    def _():
        b_first.start()

    @pl.when(rounds_second)
    def _():
        if second_at == last:
            block[...] = rblk[1]

    def relay(n, d, sign):
        kk, i = lax.rem(n, ratio), n // ratio
        h = me + sign * d
        s = h * ratio + kk
        f = s * m + i
        valid = both(n >= 0, n < flows, s >= o)
        if sign < 0:
            valid = both(valid, h >= 0)
        if sign > 0:
            valid = both(valid, h < R)
        buf = rows_at(slot0(q, s, i))

        def hop(sem, step):
            return remote(buf, buf, sem.at[f], rrecv.at[f], (col, me + step))

        deliver = remote(
            buf, rows_at(q * m + i), del_s.at[f], drecv.at[q * m + i], (s, me)
        )
        goes = col != s
        if sign == 0:
            goes = both(goes, jnp.logical_or(s != o, me != oh))
        return valid, goes, hop(up_s, 1), hop(dn_s, -1), deliver

    def relay_start(n, d, sign):
        valid, goes, up, down, deliver = relay(n, d, sign)

        @pl.when(valid)
        def _():
            up.wait_recv()
            if sign <= 0:
                @pl.when(me < R - 1)
                def _():
                    up.start()
            if sign >= 0:
                @pl.when(me > 0)
                def _():
                    down.start()

            @pl.when(goes)
            def _():
                deliver.start()

    def relay_end(n, d, sign):
        valid, goes, up, down, deliver = relay(n, d, sign)

        @pl.when(valid)
        def _():
            if sign <= 0:
                @pl.when(me < R - 1)
                def _():
                    up.wait_send()
            if sign >= 0:
                @pl.when(me > 0)
                def _():
                    down.wait_send()

            @pl.when(goes)
            def _():
                deliver.wait_send()

    def relay1(i):
        f = N * m + i
        side = jnp.where(q == lq, 0, 1)
        buf = rows_at(slot1(side, i))
        down = remote(buf, buf, dn_s.at[f], rrecv.at[f], (col, me - 1))
        j = side * m1 + i
        deliver = remote(
            buf, rows_at(n_chunks + j), del_s.at[f], qrecv.at[j], (last, me)
        )
        return down, deliver, both(me < R - 1, col != last)

    at_source = both(is_last, top)

    def relay1_start(i):
        down, deliver, goes = relay1(i)

        @pl.when(jnp.logical_not(at_source))
        def _():
            down.wait_recv()

        @pl.when(both(at_source, i == 0))
        def _():
            p1_local.wait()

        @pl.when(me > 0)
        def _():
            down.start()

        @pl.when(goes)
        def _():
            deliver.start()

    def relay1_end(i):
        down, deliver, goes = relay1(i)

        @pl.when(me > 0)
        def _():
            down.wait_send()

        @pl.when(goes)
        def _():
            deliver.wait_send()

    def walk(one, other):
        @pl.loop(0, flows + 2 * R)
        def _(level):
            for d in range(R):
                for sign in (0,) if d == 0 else (-1, 1):
                    one(level - d, d, sign)
            turn = level - (R - 1 - me)

            @pl.when(both(turn >= 0, turn < m1, jnp.logical_or(q == lq, q == nq)))
            def _():
                other(turn)

    @pl.when(carrier)
    def _():
        walk(relay_start, relay1_start)
        walk(relay_end, relay1_end)

    @pl.when(jnp.logical_not(carrier))
    def _():
        @pl.loop(0, nt)
        def _(t):
            for half in range(2):
                @pl.when(jnp.logical_or(rounds_first, spot != ends[half]))
                def _():
                    ring(t, half).wait_send()

                across(t, half).wait_send()

    @pl.when(carrier)
    def _():
        @pl.loop(0, nt)
        def _(t):
            for half in range(2):
                across(t, half).wait_recv()

    @pl.when(is_owner)
    def _():
        w_first.wait_send()
        b_first.wait_recv()

        @pl.loop(0, flows)
        def _(n):
            @pl.when(me * ratio + lax.rem(n, ratio) >= o)
            def _():
                @pl.loop(1, chips)
                def _(step):
                    scatter_to(lax.rem(oq + step, chips), n).wait_send()

    @pl.when(both(is_owner, me == oh))
    def _():
        d_first.wait_send()

    @pl.when(both(is_owner, top))
    def _():
        x_second.wait_send()

    @pl.when(rounds_first)
    def _():
        b_first.wait_send()

        @pl.when(me == oh)
        def _():
            for step in range(1, R):
                pass_diag(0, step).wait_send()

    @pl.when(both(rounds_second, top))
    def _():
        for step in range(1, R):
            pass_diag(1, step).wait_send()
            pass_cross(step).wait_send()

    if second_at != last:
        @pl.when(rounds_second)
        def _():
            @pl.loop(0, nt)
            def _(t):
                e_second(t).wait_send()
                b_second(t).wait_send()

        @pl.when(is_last)
        def _():
            w_second.wait_send()

            @pl.loop(0, nt)
            def _(t):
                e_second(t).wait_recv()
                b_second(t).wait_recv()

        @pl.when(both(is_last, top))
        def _():
            d_second.wait_send()

    @pl.when(both(is_last, top))
    def _():
        if k0 == 0:
            p1_local.wait()

        @pl.loop(0, m1)
        def _(i):
            if k0 == 0:
                scatter1(0, i).wait_send()
            scatter1(1, i).wait_send()

    @pl.loop(0, n_chunks)
    def _(j):
        carried = (j // m) * 2 + k0

        @pl.when(both(col >= o, col != carried))
        def _():
            arrived(rows_at(j), drecv.at[j]).wait_recv()

        from_other = j >= m1 if k0 == 1 else j >= 0

        @pl.when(both(is_last, me < R - 1, from_other))
        def _():
            arrived(rows_at(n_chunks + j), qrecv.at[j]).wait_recv()

    wcopy.wait()


def move(o, N, R, codes, inverse, scales, panels, weight):
    rows, cols_per = weight.shape
    chips = N // 2
    m = BLK // chips // CH
    ratio = panels.shape[1] // cols_per
    n_chunks = BLK // CH
    n_rel = N * m + n_chunks // 2
    nt = rows // ETILE
    hbm = pl.BlockSpec(memory_space=pltpu.HBM)
    vmem = pl.BlockSpec(memory_space=pltpu.VMEM)
    smem = pl.BlockSpec(memory_space=pltpu.SMEM)
    dma = pltpu.SemaphoreType.DMA
    return pl.pallas_call(
        functools.partial(move_kernel, o, N, R),
        out_shape=(
            pltpu.VMEM((2 * BLK + n_rel * CH, cols_per), F32),
            pltpu.VMEM((rows, BLK), F32),
            pltpu.VMEM((rows, BLK), F32),
            pltpu.VMEM((rows, BLK), F32),
            pltpu.VMEM((rows, cols_per), F32),
        ),
        in_specs=[smem, vmem, vmem, hbm, hbm],
        out_specs=(vmem,) * 5,
        scratch_shapes=[
            pltpu.VMEM((2, GROUPS, BLK, 8 * SUB), BF16),
            pltpu.VMEM((2, BLK, BLK), F32),
            pltpu.VMEM((BLK, BLK), F32),
            pltpu.VMEM((3 * BLK, BLK), BF16),
            pltpu.VMEM((2, rows, BLK), F32),
            pltpu.VMEM((2, rows, BLK), F32),
            dma((n_rel,)), dma((n_chunks,)), dma((n_chunks,)),
            dma((n_rel,)), dma((n_rel,)), dma((n_rel,)),
            dma((ratio * m * chips,)), dma((n_chunks,)),
            dma((nt,)), dma((nt,)), dma((nt,)), dma((nt,)), dma((nt,)), dma((nt,)),
            dma((nt,)), dma((nt,)), dma((nt,)), dma((nt,)),
            dma((2,)), dma((2 * R,)), dma, dma((R,)), dma((2,)), dma((2,)), dma((2,)), dma((2,)),
        ],
        compiler_params=pltpu.CompilerParams(
            collective_id=o + 1, has_side_effects=True, vmem_limit_bytes=18 * 1024 * 1024
        ),
        name=f"move_{o}",
    )(codes, inverse, scales[None, :], panels, weight)


def apply_kernel(o, N, col_ref, land, e0, e1, block, wv, out_ref, pcat, ecat, obuf, sems):
    rows, cols_per = wv.shape
    tile = obuf.shape[1]
    chunk = obuf.shape[2]
    slots = obuf.shape[0]
    col = col_ref[0]
    is_owner = col == o
    is_last = col == N - 1
    touched = col >= o
    nr, nc = rows // tile, cols_per // chunk

    def put_panel(b):
        @pl.loop(0, nc)
        def _(i):
            at = pl.ds(pl.multiple_of(i * chunk, chunk), chunk)
            hi, lo = split2(land[b * BLK : (b + 1) * BLK, at])
            pcat[3 * b * BLK : (3 * b + 1) * BLK, at] = hi
            pcat[(3 * b + 1) * BLK : (3 * b + 2) * BLK, at] = hi
            pcat[(3 * b + 2) * BLK : (3 * b + 3) * BLK, at] = lo

    def clear_panel(b):
        pcat[3 * b * BLK : (3 * b + 3) * BLK, :BLK] = jnp.zeros((3 * BLK, BLK), BF16)

    def put_errors(b, ref):
        hi, lo = split2(ref[...])
        ecat[:, 3 * b * BLK : (3 * b + 1) * BLK] = hi
        ecat[:, (3 * b + 1) * BLK : (3 * b + 2) * BLK] = lo
        ecat[:, (3 * b + 2) * BLK : (3 * b + 3) * BLK] = hi

    @pl.when(touched)
    def _():
        put_panel(0)
        put_errors(0, e0)

    @pl.when(is_owner)
    def _():
        clear_panel(0)

    @pl.when(is_last)
    def _():
        put_panel(1)
        clear_panel(1)
        put_errors(1, e1)

    def out_copy(step):
        slot = lax.rem(step, slots)
        c, r = step // nr, lax.rem(step, nr)
        return pltpu.make_async_copy(
            obuf.at[slot],
            out_ref.at[
                pl.ds(pl.multiple_of(r * tile, tile), tile),
                pl.ds(pl.multiple_of(c * chunk, chunk), chunk),
            ],
            sems.at[slot],
        )

    @pl.loop(0, nr * nc)
    def _(step):
        slot = lax.rem(step, slots)
        c, r = step // nr, lax.rem(step, nr)
        at_r = pl.ds(pl.multiple_of(r * tile, tile), tile)
        at_c = pl.ds(pl.multiple_of(c * chunk, chunk), chunk)

        @pl.when(step >= slots)
        def _():
            out_copy(step - slots).wait()

        @pl.when(is_last)
        def _():
            obuf[slot] = wv[at_r, at_c] - jnp.dot(
                ecat[at_r, :], pcat[:, at_c], preferred_element_type=F32
            )

        @pl.when(jnp.logical_and(touched, jnp.logical_not(is_last)))
        def _():
            obuf[slot] = wv[at_r, at_c] - jnp.dot(
                ecat[at_r, : 3 * BLK], pcat[: 3 * BLK, at_c], preferred_element_type=F32
            )

        @pl.when(jnp.logical_not(touched))
        def _():
            obuf[slot] = wv[at_r, at_c]

        @pl.when(jnp.logical_and(c == 0, jnp.logical_or(is_owner, is_last)))
        def _():
            obuf[slot, :, :BLK] = block[at_r, :]

        out_copy(step).start()

    for k in range(slots):
        out_copy(nr * nc - slots + k).wait()


def apply(o, N, col, land, e0, e1, block, wv):
    rows, cols_per = wv.shape
    tile = next(t for t in (512, 256, 128, 64, 32, 16, 8) if rows % t == 0)
    chunk = next(c for c in (512, 256, 128) if cols_per % c == 0)
    slots = 4
    vmem = pl.BlockSpec(memory_space=pltpu.VMEM)
    return pl.pallas_call(
        functools.partial(apply_kernel, o, N),
        out_shape=pltpu.HBM((rows, cols_per), F32),
        in_specs=[pl.BlockSpec(memory_space=pltpu.SMEM)] + [vmem] * 5,
        out_specs=pl.BlockSpec(memory_space=pltpu.HBM),
        scratch_shapes=[
            pltpu.VMEM((6 * BLK, cols_per), BF16),
            pltpu.VMEM((rows, 6 * BLK), BF16),
            pltpu.VMEM((slots, tile, chunk), F32),
            pltpu.SemaphoreType.DMA((slots,)),
        ],
        compiler_params=pltpu.CompilerParams(vmem_limit_bytes=18 * 1024 * 1024),
        name=f"apply_{o}",
    )(col, land, e0, e1, block, wv)


def local(N, R, weight, scales, panels, block_inverse, grid_codes, block_starts):
    cols_per = weight.shape[1]
    owner = block_starts[0] // cols_per

    def branch(o):
        def run(weight, scales, panels, inverse, codes):
            parts = move(o, N, R, codes, inverse, scales, panels, weight)
            col = lax.axis_index("cols").astype(jnp.int32)[None]
            parts = [pltpu.with_memory_space_constraint(x, pltpu.VMEM) for x in parts]
            return apply(o, N, col, *parts)
        return run

    return lax.switch(
        owner, [branch(o) for o in range(N - 1)],
        weight, scales, panels, block_inverse, grid_codes,
    )


def solution(mesh):
    N, R = mesh.shape["cols"], mesh.shape["rows"]
    placed = (P("rows", "cols"), P("rows"), P("cols", "rows"), P(), P(), P())
    return jax.shard_map(
        functools.partial(local, N, R), mesh=mesh, in_specs=placed,
        out_specs=P("rows", "cols"), check_vma=False,
    )
```
